8 devices in a mesh: rep: 1 (over z), dp: 8 (over x, y, core).
Axes of the slice: x: 2, y: 2, z: 1, core: 2. Of those that a mesh axis runs over, the one named last changes fastest.
Arguments:
- x: bfloat16 [8, 2048, 1024], P(('rep', 'dp'))
- dy: bfloat16 [8, 2048, 1024], P(('rep', 'dp'))
- wq: bfloat16 [2, 1024, 1024], P(None, 'dp')
- wk: bfloat16 [2, 1024, 1024], P(None, 'dp')
- wv: bfloat16 [2, 1024, 1024], P(None, 'dp')
- wo: bfloat16 [2, 1024, 1024], P(None, 'dp')
- w_gate: bfloat16 [2, 1024, 4096], P(None, 'dp')
- w_up: bfloat16 [2, 1024, 4096], P(None, 'dp')
- w_down: bfloat16 [2, 4096, 1024], P(None, 'dp')
- m_wq: float32 [2, 1024, 1024], P(None, 'dp')
- m_wk: float32 [2, 1024, 1024], P(None, 'dp')
- m_wv: float32 [2, 1024, 1024], P(None, 'dp')
- m_wo: float32 [2, 1024, 1024], P(None, 'dp')
- m_w_gate: float32 [2, 1024, 4096], P(None, 'dp')
- m_w_up: float32 [2, 1024, 4096], P(None, 'dp')
- m_w_down: float32 [2, 4096, 1024], P(None, 'dp')
- v_wq: float32 [2, 1024, 1024], P(None, 'dp')
- v_wk: float32 [2, 1024, 1024], P(None, 'dp')
- v_wv: float32 [2, 1024, 1024], P(None, 'dp')
- v_wo: float32 [2, 1024, 1024], P(None, 'dp')
- v_w_gate: float32 [2, 1024, 4096], P(None, 'dp')
- v_w_up: float32 [2, 1024, 4096], P(None, 'dp')
- v_w_down: float32 [2, 4096, 1024], P(None, 'dp')
Outputs:
- output 1: bfloat16 [2, 1024, 1024], P('rep', 'dp')
- output 2: bfloat16 [2, 1024, 1024], P('rep', 'dp')
- output 3: bfloat16 [2, 1024, 1024], P('rep', 'dp')
- output 4: bfloat16 [2, 1024, 1024], P('rep', 'dp')
- output 5: bfloat16 [2, 1024, 4096], P('rep', 'dp')
- output 6: bfloat16 [2, 1024, 4096], P('rep', 'dp')
- output 7: bfloat16 [2, 4096, 1024], P('rep', 'dp')
- output 8: float32 [2, 1024, 1024], P('rep', 'dp')
- output 9: float32 [2, 1024, 1024], P('rep', 'dp')
- output 10: float32 [2, 1024, 1024], P('rep', 'dp')
- output 11: float32 [2, 1024, 1024], P('rep', 'dp')
- output 12: float32 [2, 1024, 4096], P('rep', 'dp')
- output 13: float32 [2, 1024, 4096], P('rep', 'dp')
- output 14: float32 [2, 4096, 1024], P('rep', 'dp')
- output 15: float32 [2, 1024, 1024], P('rep', 'dp')
- output 16: float32 [2, 1024, 1024], P('rep', 'dp')
- output 17: float32 [2, 1024, 1024], P('rep', 'dp')
- output 18: float32 [2, 1024, 1024], P('rep', 'dp')
- output 19: float32 [2, 1024, 4096], P('rep', 'dp')
- output 20: float32 [2, 1024, 4096], P('rep', 'dp')
- output 21: float32 [2, 4096, 1024], P('rep', 'dp')
All inputs are finite; a program needn't handle non-finite values.
Results may differ from the reference program's by a relative error of at most 0.024.
Values are sent between devices in bfloat16 or wider.
A program may use at most 2 GiB of HBM per device.

```python
import jax
import jax.numpy as jnp
from jax import lax

SEQUENCES = 8
TOKENS = 2048
D = 1024
HEADS = 4
KV_HEADS = 4
HEAD = 256
FF = 4096
LAYERS = 2
THETA = 10000
NAMES = ("wq", "wk", "wv", "wo", "w_gate", "w_up", "w_down")
SHAPES = {
    "wq": (LAYERS, D, HEADS * HEAD),
    "wk": (LAYERS, D, KV_HEADS * HEAD),
    "wv": (LAYERS, D, KV_HEADS * HEAD),
    "wo": (LAYERS, HEADS * HEAD, D),
    "w_gate": (LAYERS, D, FF),
    "w_up": (LAYERS, D, FF),
    "w_down": (LAYERS, FF, D),
}


def bump(key, n, height):
    away = (jnp.arange(n, dtype=jnp.int32) - jax.random.randint(key, (), 0, n, jnp.int32)) % n
    return jnp.where(away < n // 8, height, 1.0)


def together(key, own, strength):
    shared = jax.random.normal(key, own.shape[1:], jnp.float32)
    return (own + strength * shared) * lax.rsqrt(1 + strength * strength)


def setup_inputs(seed: int = 0, part: int = 0) -> dict:
    kx, kdy, ka, kb, kz, kf, kh, kl, *keys = jax.random.split(jax.random.key(seed), 8 + 3 * len(NAMES))
    kx, kdy, ka, kb = (jax.random.fold_in(k, part) for k in (kx, kdy, ka, kb))
    kw, km, kv = (keys[i::3] for i in range(3))
    shape = (SEQUENCES, TOKENS, D)
    much_x, much_dy = jax.random.uniform(kz, (2,), jnp.float32, 0.0, 1.0)
    loud = 2.0 ** jax.random.uniform(jax.random.fold_in(kz, 1), (), jnp.float32, -1.0, 2.0)
    layers = 2.0 ** jax.random.uniform(kl, (LAYERS, 1, 1), jnp.float32, -1.0, 1.0)
    times = {"wq": 1.0, "wk": 1.0, "wv": 2.0, "wo": layers, "w_gate": 1.0, "w_up": bump(kh, FF, 4.0), "w_down": layers}
    x = together(ka, jax.random.normal(kx, shape, jnp.float32), much_x) * bump(kf, D, 4.0)
    dy = together(kb, jax.random.normal(kdy, shape, jnp.float32), much_dy)
    drawn = {"x": x.astype(jnp.bfloat16), "dy": (loud * dy * (SEQUENCES * TOKENS) ** -0.5).astype(jnp.bfloat16)}
    for key, name in zip(kw, NAMES, strict=True):
        drawn[name] = (jax.random.normal(key, SHAPES[name], jnp.float32) * SHAPES[name][1] ** -0.5 * times[name]).astype(jnp.bfloat16)
    for key, name in zip(km, NAMES, strict=True):
        drawn[f"m_{name}"] = 0.1 * jax.random.normal(key, SHAPES[name], jnp.float32)
    for key, name in zip(kv, NAMES, strict=True):
        drawn[f"v_{name}"] = jax.random.uniform(key, SHAPES[name], jnp.float32, 0.02, 0.06)
    return drawn


def matmul(a, w):
    return jnp.dot(a, w, preferred_element_type=jnp.float32).astype(jnp.bfloat16)


def normed(h):
    wide = h.astype(jnp.float32)
    scale = lax.rsqrt(jnp.mean(wide**2, -1, keepdims=True) + 1e-6)
    return (wide * scale).astype(jnp.bfloat16)


def turned(t, theta):
    half = t.shape[-1] // 2
    angle = jnp.arange(t.shape[0], dtype=jnp.float32)[:, None] * theta ** (-jnp.arange(half, dtype=jnp.float32) / half)
    cos, sin = jnp.cos(angle)[:, None], jnp.sin(angle)[:, None]
    a, b = t[..., :half].astype(jnp.float32), t[..., half:].astype(jnp.float32)
    return jnp.concatenate([a * cos - b * sin, b * cos + a * sin], -1).astype(jnp.bfloat16)


def seen_by(q, k, v):
    tokens, kv = q.shape[0], k.shape[1]
    q = q.reshape(tokens, kv, -1, q.shape[-1])
    scores = jnp.einsum("tgsd,ugd->gstu", q.astype(jnp.float32), k.astype(jnp.float32)) * q.shape[-1] ** -0.5
    place = jnp.arange(tokens)
    weights = jax.nn.softmax(jnp.where(place[:, None] >= place, scores, -jnp.inf), -1).astype(jnp.bfloat16)
    return jnp.einsum("gstu,ugd->tgsd", weights.astype(jnp.float32), v.astype(jnp.float32)).astype(jnp.bfloat16).reshape(tokens, -1)


def layer(h, w):
    a = normed(h)
    q, k = (turned(matmul(a, w[name]).reshape(h.shape[0], -1, HEAD), THETA) for name in ("wq", "wk"))
    h = h + matmul(seen_by(q, k, matmul(a, w["wv"]).reshape(h.shape[0], -1, HEAD)), w["wo"])
    b = normed(h)
    gate = jnp.dot(b, w["w_gate"], preferred_element_type=jnp.float32)
    up = jnp.dot(b, w["w_up"], preferred_element_type=jnp.float32)
    return h + matmul((jax.nn.silu(gate) * up).astype(jnp.bfloat16), w["w_down"])


def adamw(w, m, v, g):
    m = 0.9 * m + 0.1 * g
    v = 0.95 * v + 0.05 * g * g
    step = m * lax.rsqrt(v + 1e-8) + 0.1 * w
    return (w - 0.02 * step).astype(jnp.bfloat16), m, v


def clipped(gradients, sum_of_squares, count):
    factor = jnp.minimum(1.0, 0.5 * lax.rsqrt(sum_of_squares / count + 1e-30))
    return [g * factor for g in gradients]


def stack(weights, h):
    return lax.scan(lambda h, w: (layer(h, w), None), h, weights)[0]


def reference(x, dy, wq, wk, wv, wo, w_gate, w_up, w_down, m_wq, m_wk, m_wv, m_wo, m_w_gate, m_w_up, m_w_down, v_wq, v_wk, v_wv, v_wo, v_w_gate, v_w_up, v_w_down):
    weights = dict(zip(NAMES, (wq, wk, wv, wo, w_gate, w_up, w_down), strict=True))

    def take(so_far, sequence):
        h, by_y = sequence
        _, back = jax.vjp(stack, weights, h)
        by_weights, by_h = back(by_y)
        return jax.tree.map(lambda total, term: total + term.astype(jnp.float32), so_far, by_weights), by_h

    none_yet = {name: jnp.zeros(w.shape, jnp.float32) for name, w in weights.items()}
    by_weights, by_x = lax.scan(take, none_yet, (x, dy))
    gradients = [by_weights[name].astype(jnp.bfloat16).astype(jnp.float32) for name in NAMES]
    gradients = clipped(gradients, sum(jnp.sum(g * g) for g in gradients), sum(g.size for g in gradients))
    first = (m_wq, m_wk, m_wv, m_wo, m_w_gate, m_w_up, m_w_down)
    second = (v_wq, v_wk, v_wv, v_wo, v_w_gate, v_w_up, v_w_down)
    new = [adamw(weights[name].astype(jnp.float32), m, v, g) for name, m, v, g in zip(NAMES, first, second, gradients, strict=True)]
    return tuple(one[which] for which in range(3) for one in new)
```

```python
import functools

import jax
import jax.numpy as jnp
from jax import lax
from jax.experimental import pallas as pl
from jax.experimental.pallas import tpu as pltpu
from jax.sharding import PartitionSpec as P

NEG = -1e30
HIDDEN = 2 * NEG
LOG2E = 1.4426950408889634
VMEM = 62 * 2**20
HEAD = 256
HALF = HEAD // 2
THETA = 10000
NAMES = ("wq", "wk", "wv", "wo", "w_gate", "w_up", "w_down")
BF, F32 = jnp.bfloat16, jnp.float32
ROWS = 512
WIDE = 1024


def _nn(a, b):
    return lax.dot_general(a, b, (((1,), (0,)), ((), ())), preferred_element_type=F32)


def _nt(a, b):
    return lax.dot_general(a, b, (((1,), (1,)), ((), ())), preferred_element_type=F32)


def _low(x):
    return x.astype(BF)


def _round(x):
    return x.astype(BF).astype(F32)


def _scale(wide):
    return lax.rsqrt(jnp.mean(wide * wide, -1, keepdims=True) + 1e-6)


def _norm_back(by_b, wide):
    scale = _scale(wide)
    by_scale = jnp.sum(by_b * wide, -1, keepdims=True)
    return by_b * scale - wide * (scale * scale * scale * by_scale * (1 / wide.shape[-1]))


def _turn(t, cos, sin):
    a, b = t[:, :HALF], t[:, HALF:]
    return jnp.concatenate([a * cos - b * sin, b * cos + a * sin], -1)


def _rows(shape):
    return pl.BlockSpec(shape, lambda i, *_: (i, 0))


def _held(w):
    _, rows, columns, at = w
    return pl.BlockSpec((rows, columns), lambda *_: (0, at), pipeline_mode=pl.Buffered(1))


def _call(body, grid, ins, outs, flops, scratch=(), name=None, order=None):
    size = lambda s, d: int(jnp.dtype(d).itemsize) * functools.reduce(lambda a, b: a * b, s, 1)
    moved = sum(size(a.shape, a.dtype) for a, _ in ins) + sum(size(s, d) for s, d, _ in outs)
    return pl.pallas_call(
        body,
        grid=grid,
        in_specs=[s for _, s in ins],
        out_specs=[s for _, _, s in outs],
        out_shape=[jax.ShapeDtypeStruct(s, d) for s, d, _ in outs],
        scratch_shapes=list(scratch),
        compiler_params=pltpu.CompilerParams(dimension_semantics=("arbitrary",) * len(grid), vmem_limit_bytes=VMEM),
        cost_estimate=pl.CostEstimate(flops=flops, transcendentals=0, bytes_accessed=moved),
        name=name,
    )(*(a for a, _ in ins))


def _qkv_body(h_ref, cos_ref, sin_ref, wq, wk, wv, a_ref, q_ref, k_ref, v_ref):
    wide = h_ref[...].astype(F32)
    a = _low(wide * _scale(wide))
    a_ref[...] = a
    cos, sin = cos_ref[...], sin_ref[...]
    for w, out, turned in ((wq, q_ref, True), (wk, k_ref, True), (wv, v_ref, False)):
        for at in range(0, w.shape[1], HEAD):
            y = _low(_nn(a, w[:, at : at + HEAD]))
            out[:, at : at + HEAD] = _low(_turn(y.astype(F32), cos, sin)) if turned else y


def fwd_qkv(h, cos, sin, wq, wk, wv):
    s, d = h.shape
    n = wq[2]
    blk = lambda c: _rows((ROWS, c))
    return _call(_qkv_body, (s // ROWS,), [(h, blk(d)), (cos, blk(HALF)), (sin, blk(HALF))] + [(w[0], _held(w)) for w in (wq, wk, wv)],
                 [((s, d), BF, blk(d))] + [((s, n), BF, blk(n))] * 3, 6 * s * d * n, name="qkv")


def _attn_body(q_ref, k_ref, v_ref, o_ref, lse_ref, top_s, mix_s, *, scale, bq, bk, heads):
    iq = pl.program_id(0)
    e = scale * LOG2E
    for i in range(heads):
        top_s[i : i + 1, :] = jnp.full((1, bq), NEG, F32)
        mix_s[i] = jnp.zeros((HEAD + 8, bq), F32)
    ones = jnp.ones((8, bk), BF)

    def block(first, lo, diagonal):
        here = pl.ds(first, bk)
        spans = [(lo, bk, True)] + ([(lo + bk, bq - lo - bk, False)] if lo + bk < bq else []) if diagonal else [(0, bq, False)]
        pieces = [(i, *span) for i in range(heads) for span in spans]
        scores = [_nt(k_ref[here, i * HEAD : (i + 1) * HEAD], q_ref[at : at + n, i * HEAD : (i + 1) * HEAD]) for i, at, n, _ in pieces]
        weights, keeps = [], []
        for (i, at, n, masked), s in zip(pieces, scores):
            if masked:
                ok = lax.broadcasted_iota(jnp.int32, (bk, n), 1) >= lax.broadcasted_iota(jnp.int32, (bk, n), 0)
                s = jnp.where(ok, s, HIDDEN)
            old = top_s[i : i + 1, at : at + n]
            top = jnp.maximum(old, s.max(axis=0, keepdims=True))
            top_s[i : i + 1, at : at + n] = top
            weights.append(_low(jnp.exp2((s - top) * e)))
            keeps.append(jnp.exp2((old - top) * e))
        for (i, at, n, _), p, keep in zip(pieces, weights, keeps):
            values = jnp.concatenate([v_ref[here, i * HEAD : (i + 1) * HEAD].T, ones], axis=0)
            mix_s[i, :, at : at + n] = mix_s[i, :, at : at + n] * keep + _nn(values, p)

    lax.fori_loop(0, iq * (bq // bk), lambda j, _: block(pl.multiple_of(j * bk, bk), 0, False), None)
    for t in range(bq // bk):
        block(pl.multiple_of(iq * bq + t * bk, bk), t * bk, True)
    for i in range(heads):
        top, total = top_s[i : i + 1, :], mix_s[i, HEAD : HEAD + 1, :]
        o_ref[:, i * HEAD : (i + 1) * HEAD] = _low((mix_s[i, :HEAD, :] * (1 / total)).T)
        lse_ref[i : i + 1, :] = top * scale + jnp.log(total)


FWD_BQ, FWD_BK = 512, 512
BWD_BQ, BWD_BK = 512, 512


def attend(q, k, v):
    s, n = q.shape
    heads, bq, bk = n // HEAD, FWD_BQ, FWD_BK
    whole = pl.BlockSpec((s, n), lambda i: (0, 0), pipeline_mode=pl.Buffered(1))
    return _call(functools.partial(_attn_body, scale=HEAD**-0.5, bq=bq, bk=bk, heads=heads), (s // bq,),
                 [(q, _rows((bq, n))), (k, whole), (v, whole)],
                 [((s, n), BF, _rows((bq, n))), ((heads, s), F32, pl.BlockSpec((heads, bq), lambda i: (0, i)))], 4 * s * s * n,
                 [pltpu.VMEM((heads, bq), F32), pltpu.VMEM((heads, HEAD + 8, bq), F32)], name="attend")


def _out_body(o_ref, h_ref, wo, h2_ref, b_ref):
    h2 = _low(h_ref[...].astype(F32) + _round(_nn(o_ref[...], wo[...])))
    h2_ref[...] = h2
    wide = h2.astype(F32)
    b_ref[...] = _low(wide * _scale(wide))


def fwd_out(o, h, wo):
    s, d = h.shape
    n = o.shape[1]
    return _call(_out_body, (s // ROWS,), [(o, _rows((ROWS, n))), (h, _rows((ROWS, d))), (wo[0], _held(wo))],
                 [((s, d), BF, _rows((ROWS, d)))] * 2, 2 * s * d * n, name="out")


def _gate_up_body(b_ref, wg, wu, act_ref, by_up_ref, by_gate_ref):
    here = pl.ds(pl.multiple_of(pl.program_id(1) * WIDE, WIDE), WIDE)
    b = b_ref[...]
    gate, up = _nn(b, wg[:, here]), _nn(b, wu[:, here])
    sig = jax.nn.sigmoid(gate)
    silu = gate * sig
    act_ref[...] = _low(silu * up)
    by_up_ref[...] = silu
    by_gate_ref[...] = up * (sig + silu * (1 - sig))


def fwd_gate_up(b, wg, wu):
    s, d = b.shape
    f = wg[2]
    blk = pl.BlockSpec((ROWS, WIDE), lambda i, j: (i, j))
    return _call(_gate_up_body, (s // ROWS, f // WIDE), [(b, _rows((ROWS, d))), (wg[0], _held(wg)), (wu[0], _held(wu))],
                 [((s, f), BF, blk), ((s, f), F32, blk), ((s, f), F32, blk)], 4 * s * d * f, name="gate_up")


def _down_body(act_ref, h_ref, wd, out_ref):
    out_ref[...] = _low(h_ref[...].astype(F32) + _round(_nn(act_ref[...], wd[...])))


def fwd_down(act, h2, wd):
    s, d = h2.shape
    f = act.shape[1]
    return _call(_down_body, (s // ROWS,), [(act, _rows((ROWS, f))), (h2, _rows((ROWS, d))), (wd[0], _held(wd))],
                 [((s, d), BF, _rows((ROWS, d)))], 2 * s * d * f, name="down")[0]


def _mlp_back_body(dy_ref, by_up_ref, by_gate_ref, h2_ref, o_ref, wd, wg, wu, wo, dg_ref, du_ref, dh_ref, do_ref, delta_ref, acc_g, acc_u):
    c = pl.program_id(1)
    here = pl.ds(pl.multiple_of(c * WIDE, WIDE), WIDE)
    dact = _round(_nt(dy_ref[...], wd[here, :]))
    du, dg = _low(dact * by_up_ref[...]), _low(dact * by_gate_ref[...])
    du_ref[...], dg_ref[...] = du, dg
    to_g, to_u = _nt(dg, wg[:, here]), _nt(du, wu[:, here])

    @pl.when(c == 0)
    def _():
        acc_g[...], acc_u[...] = to_g, to_u

    @pl.when(c > 0)
    def _():
        acc_g[...] += to_g
        acc_u[...] += to_u

    @pl.when(c == pl.num_programs(1) - 1)
    def _():
        by_b = _round(_round(acc_g[...]) + _round(acc_u[...]))
        dh = _low(dy_ref[...].astype(F32) + _round(_norm_back(by_b, h2_ref[...].astype(F32))))
        dh_ref[...] = dh
        do = _low(_nt(dh, wo[...]))
        do_ref[...] = do
        both = do.astype(F32) * o_ref[...].astype(F32)
        for i in range(both.shape[1] // HEAD):
            delta_ref[i : i + 1, :] = jnp.sum(both[:, i * HEAD : (i + 1) * HEAD].T, axis=0, keepdims=True)


def mlp_back(dy, by_up, by_gate, h2, o, wd, wg, wu, wo):
    s, d = dy.shape
    f, n = wg[2], o.shape[1]
    row = lambda c: _rows((ROWS, c))
    blk = pl.BlockSpec((ROWS, WIDE), lambda i, j: (i, j))
    return _call(_mlp_back_body, (s // ROWS, f // WIDE),
                 [(dy, row(d)), (by_up, blk), (by_gate, blk), (h2, row(d)), (o, row(n))] + [(w[0], _held(w)) for w in (wd, wg, wu, wo)],
                 [((s, f), BF, blk), ((s, f), BF, blk), ((s, d), BF, row(d)), ((s, n), BF, row(n)),
                  ((n // HEAD, s), F32, pl.BlockSpec((n // HEAD, ROWS), lambda i, j: (0, i)))],
                 6 * s * d * f + 2 * s * d * n, [pltpu.VMEM((ROWS, d), F32)] * 2, name="mlp_back")


def _attn_back_body(q_ref, k_ref, v_ref, do_ref, lse_ref, delta_ref, cosq_ref, sinq_ref, cos_ref, sin_ref, dq_ref, dk_ref, dv_ref,
                    dq_s, dk_s, dv_s, *, scale, bq, bk, heads):
    iq = pl.program_id(1)
    e = scale * LOG2E

    @pl.when(iq == 0)
    def _():
        dk_s[...] = jnp.zeros_like(dk_s)
        dv_s[...] = jnp.zeros_like(dv_s)

    dq_s[...] = jnp.zeros_like(dq_s)
    lses = [lse_ref[0, i : i + 1, :] * LOG2E for i in range(heads)]
    deltas = [delta_ref[0, i : i + 1, :] for i in range(heads)]

    def block(first, lo, diagonal):
        here = pl.ds(first, bk)
        spans = [(lo, bk, True)] + ([(lo + bk, bq - lo - bk, False)] if lo + bk < bq else []) if diagonal else [(0, bq, False)]
        pieces = [(i, *span) for i in range(heads) for span in spans]
        col = lambda i: slice(i * HEAD, (i + 1) * HEAD)
        qs = [q_ref[at : at + n, col(i)] for i, at, n, _ in pieces]
        dos = [do_ref[at : at + n, col(i)] for i, at, n, _ in pieces]
        scores = [_nt(k_ref[here, col(p[0])], x) for p, x in zip(pieces, qs)]
        dps = [_nt(v_ref[here, col(p[0])], x) for p, x in zip(pieces, dos)]
        for m, (i, at, n, masked) in enumerate(pieces):
            p = jnp.exp2(scores[m] * e - lses[i][:, at : at + n])
            if masked:
                ok = lax.broadcasted_iota(jnp.int32, (bk, n), 1) >= lax.broadcasted_iota(jnp.int32, (bk, n), 0)
                p = jnp.where(ok, p, 0.0)
            ds = _low(p * (dps[m] - deltas[i][:, at : at + n]))
            dv_s[here, col(i)] += _nn(_low(p), dos[m])
            dk_s[here, col(i)] += _nn(ds, qs[m])
            dq_s[i, :, at : at + n] += _nn(k_ref[here, col(i)].T, ds)

    lax.fori_loop(0, iq * (bq // bk), lambda j, _: block(pl.multiple_of(j * bk, bk), 0, False), None)
    for t in range(bq // bk):
        block(pl.multiple_of(iq * bq + t * bk, bk), t * bk, True)
    for i in range(heads):
        dq_ref[:, i * HEAD : (i + 1) * HEAD] = _low(_turn(_round((dq_s[i] * scale).T), cosq_ref[...], -sinq_ref[...]))

    @pl.when(iq == pl.num_programs(1) - 1)
    def _():
        for i in range(heads):
            dk_ref[:, i * HEAD : (i + 1) * HEAD] = _low(_turn(_round(dk_s[:, i * HEAD : (i + 1) * HEAD] * scale), cos_ref[...], -sin_ref[...]))
            dv_ref[:, i * HEAD : (i + 1) * HEAD] = _low(dv_s[:, i * HEAD : (i + 1) * HEAD])


def attend_back(q, k, v, do, lse, delta, cos, sin):
    s, n = q.shape
    kb, bq, bk = 2, BWD_BQ, BWD_BK
    w, groups = kb * HEAD, n // HEAD // kb
    part = pl.BlockSpec((bq, w), lambda g, i: (i, g))
    whole = pl.BlockSpec((s, w), lambda g, i: (0, g))
    stats = pl.BlockSpec((1, kb, bq), lambda g, i: (g, 0, i))
    table = pl.BlockSpec((s, HALF), lambda g, i: (0, 0), pipeline_mode=pl.Buffered(1))
    near = pl.BlockSpec((bq, HALF), lambda g, i: (i, 0))
    return _call(functools.partial(_attn_back_body, scale=HEAD**-0.5, bq=bq, bk=bk, heads=kb), (groups, s // bq),
                 [(q, part), (k, whole), (v, whole), (do, part), (lse.reshape(groups, kb, s), stats), (delta.reshape(groups, kb, s), stats),
                  (cos, near), (sin, near), (cos, table), (sin, table)],
                 [((s, n), BF, part), ((s, n), BF, whole), ((s, n), BF, whole)], 5 * s * s * n,
                 [pltpu.VMEM((kb, HEAD, bq), F32), pltpu.VMEM((s, w), F32), pltpu.VMEM((s, w), F32)], name="attend_back")


def _qkv_back_body(dq_ref, dk_ref, dv_ref, h_ref, dh_ref, wq, wk, wv, out_ref):
    by_a = _round(_nt(dq_ref[...], wq[...])) + _round(_nt(dk_ref[...], wk[...]))
    by_a = _round(_round(by_a) + _round(_nt(dv_ref[...], wv[...])))
    out_ref[...] = _low(dh_ref[...].astype(F32) + _round(_norm_back(by_a, h_ref[...].astype(F32))))


def qkv_back(dq, dk, dv, h, dh, wq, wk, wv):
    s, d = h.shape
    n = dq.shape[1]
    return _call(_qkv_back_body, (s // ROWS,), [(x, _rows((ROWS, x.shape[1]))) for x in (dq, dk, dv, h, dh)] + [(w[0], _held(w)) for w in (wq, wk, wv)],
                 [((s, d), BF, _rows((ROWS, d)))], 6 * s * d * n, name="qkv_back")[0]


def _weight_back_body(*refs, plan, per):
    count = len(plan)
    a_refs, b_refs, out_ref, a_s = refs[: max(plan) + 1], refs[-count - 2 : -2], refs[-2], refs[-1]
    j = pl.program_id(0)
    for i, which in enumerate(plan):
        if i == 0 or plan[i - 1] != which:
            @pl.when(j == i * per)
            def _():
                a_s[...] = a_refs[which][...].T

        @pl.when((j >= i * per) & (j < (i + 1) * per))
        def _():
            out_ref[...] = _low(_nn(a_s[...], b_refs[i][...]))


def weight_back(pairs, wide=512):
    firsts, plan = [], []
    for a, _ in pairs:
        if not any(a is x for x in firsts):
            firsts.append(a)
        plan.append([a is x for x in firsts].index(True))
    bs = [b for _, b in pairs]
    (s, m), n = firsts[0].shape, bs[0].shape[1]
    per = n // wide
    spec = lambda i: pl.BlockSpec((s, wide), lambda j: (0, jnp.clip(j - i * per, 0, per - 1)))
    return _call(functools.partial(_weight_back_body, plan=plan, per=per), (per * len(bs),),
                 [(a, pl.BlockSpec((s, m), lambda j: (0, 0), pipeline_mode=pl.Buffered(1))) for a in firsts] + [(b, spec(i)) for i, b in enumerate(bs)],
                 [((m, n * len(bs)), BF, pl.BlockSpec((m, wide), lambda j: (0, j)))], 2 * s * m * n * len(bs), [pltpu.VMEM((m, s), BF)], name="weight_back")[0]


def _tall_back_body(a_ref, b_ref, out_ref):
    out_ref[...] = _low(_nn(a_ref[...].T, b_ref[...]))


def tall_back(a, b, tall=512):
    (s, m), n = a.shape, b.shape[1]
    return _call(_tall_back_body, (m // tall,),
                 [(a, pl.BlockSpec((s, tall), lambda j: (0, j))), (b, pl.BlockSpec((s, n), lambda j: (0, 0), pipeline_mode=pl.Buffered(1)))],
                 [((m, n), BF, pl.BlockSpec((tall, n), lambda j: (j, 0)))], 2 * s * m * n, name="tall_back")[0]


def adamw(w, m, v, g):
    m = 0.9 * m + 0.1 * g
    v = 0.95 * v + 0.05 * g * g
    step = m * lax.rsqrt(v + 1e-8) + 0.1 * w
    return (w - 0.02 * step).astype(BF), m, v


def solution(mesh):
    def gathered(*parts):
        whole = lax.all_gather(parts[0] if len(parts) == 1 else jnp.concatenate(parts, axis=1), "dp", axis=0, tiled=True)
        return whole

    def scattered(g):
        return lax.psum_scatter(g, "dp", scatter_dimension=0, tiled=True)

    def step(x, dy, *arrays):
        weights, m, v = (arrays[i : i + 7] for i in (0, 7, 14))
        sharded = [dict(zip(NAMES, [w[number] for w in weights])) for number in range(2)]
        s, d = x.shape[1:]
        f = weights[4].shape[2]
        angle = jnp.arange(s, dtype=F32)[:, None] * THETA ** (-jnp.arange(HALF, dtype=F32) / HALF)
        cos, sin = jnp.cos(angle), jnp.sin(angle)

        n = weights[0].shape[2]
        full = []
        for number in range(2):
            w = sharded[number]
            qkvo = gathered(*(w[name] for name in NAMES[:4]))
            gu = gathered(w["w_gate"], w["w_up"])
            down = gathered(w["w_down"])
            got = {name: (qkvo, d, n, i) for i, name in enumerate(NAMES[:4])}
            got.update(w_gate=(gu, d, f, 0), w_up=(gu, d, f, 1), w_down=(down, f, d, 0))
            full.append(got)

        h, kept = x[0], []
        for w in full:
            a, q, k, vv = fwd_qkv(h, cos, sin, w["wq"], w["wk"], w["wv"])
            o, lse = attend(q, k, vv)
            h2, b = fwd_out(o, h, w["wo"])
            act, by_up, by_gate = fwd_gate_up(b, w["w_gate"], w["w_up"])
            kept.append((h, a, q, k, vv, o, lse, h2, b, act, by_up, by_gate))
            if w is not full[-1]:
                h = fwd_down(act, h2, w["w_down"])

        by_h, mine = dy[0], [None, None]
        tie = lambda *xs: lax.optimization_barrier(xs)
        last = None
        for number in (1, 0):
            w = full[number]
            h, a, q, k, vv, o, lse, h2, b, act, by_up, by_gate = kept[number]
            g_down = tall_back(act, by_h)
            g_down, by_h = tie(g_down, by_h)
            s_down = scattered(g_down)
            dg, du, dh, do, delta = mlp_back(by_h, by_up, by_gate, h2, o, w["w_down"], w["w_gate"], w["w_up"], w["wo"])
            if number == 0:
                s_gu1, dg = tie(s_gu, dg)
            g_gu = weight_back([(b, dg), (b, du)])
            if number == 0:
                s_qkvo1, g_gu, do = tie(s_qkvo, g_gu, do)
            else:
                g_gu, do = tie(g_gu, do)
            s_gu = scattered(g_gu)
            dq, dk, dv = attend_back(q, k, vv, do, lse, delta, cos, sin)
            s_down, dq = tie(s_down, dq)
            g_qkvo = weight_back([(a, dq), (a, dk), (a, dv), (o, dh)])
            if number:
                g_qkvo, dq = tie(g_qkvo, dq)
                s_down1 = s_down
                by_h = qkv_back(dq, dk, dv, h, dh, w["wq"], w["wk"], w["wv"])
            else:
                s_gu, g_qkvo = tie(s_gu, g_qkvo)
            s_qkvo = scattered(g_qkvo)
        parts = ((s_qkvo, s_gu, s_down), (s_qkvo1, s_gu1, s_down1))
        for number, (one, two, three) in enumerate(parts):
            mine[number] = [one[:, i * n : (i + 1) * n] for i in range(4)] + [two[:, :f], two[:, f:], three]

        squares = lax.psum(sum(jnp.sum(jnp.square(g.astype(F32))) for layer in mine for g in layer), "dp")
        count = lax.psum(1, "dp") * sum(g.size for layer in mine for g in layer)
        factor = jnp.minimum(1.0, 0.5 * lax.rsqrt(squares / count + 1e-30))
        gradients = [jnp.stack([mine[0][i], mine[1][i]]).astype(F32) * factor for i in range(7)]
        new = [adamw(w.astype(F32), m, v, g) for w, m, v, g in zip(weights, m, v, gradients, strict=True)]
        return tuple(one[which] for which in range(3) for one in new)

    states, cut = P(("rep", "dp"), None, None), P(None, "dp", None)
    return jax.shard_map(
        step,
        mesh=mesh,
        in_specs=(states, states) + (cut,) * 21,
        out_specs=(P("rep", "dp", None),) * 21,
        check_vma=False,
    )
```

```python
import functools

import jax
import jax.numpy as jnp
from jax import lax
from jax.experimental import pallas as pl
from jax.experimental.pallas import tpu as pltpu
from jax.sharding import PartitionSpec as P

NEG = -1e30
HIDDEN = 2 * NEG
LOG2E = 1.4426950408889634
VMEM = 62 * 2**20
HEAD = 256
HALF = HEAD // 2
THETA = 10000
NAMES = ("wq", "wk", "wv", "wo", "w_gate", "w_up", "w_down")
BF, F32 = jnp.bfloat16, jnp.float32
ROWS = 512
WIDE = 1024


def _nn(a, b):
    return lax.dot_general(a, b, (((1,), (0,)), ((), ())), preferred_element_type=F32)


def _nt(a, b):
    return lax.dot_general(a, b, (((1,), (1,)), ((), ())), preferred_element_type=F32)


def _low(x):
    return x.astype(BF)


def _round(x):
    return x.astype(BF).astype(F32)


def _scale(wide):
    return lax.rsqrt(jnp.mean(wide * wide, -1, keepdims=True) + 1e-6)


def _norm_back(by_b, wide):
    scale = _scale(wide)
    by_scale = jnp.sum(by_b * wide, -1, keepdims=True)
    return by_b * scale - wide * (scale * scale * scale * by_scale * (1 / wide.shape[-1]))


def _turn(t, cos, sin):
    a, b = t[:, :HALF], t[:, HALF:]
    return jnp.concatenate([a * cos - b * sin, b * cos + a * sin], -1)


def _rows(shape):
    return pl.BlockSpec(shape, lambda i, *_: (i, 0))


def _held(w):
    _, rows, columns, at = w
    return pl.BlockSpec((rows, columns), lambda *_: (0, at), pipeline_mode=pl.Buffered(1))


def _call(body, grid, ins, outs, flops, scratch=(), name=None, order=None):
    size = lambda s, d: int(jnp.dtype(d).itemsize) * functools.reduce(lambda a, b: a * b, s, 1)
    moved = sum(size(a.shape, a.dtype) for a, _ in ins) + sum(size(s, d) for s, d, _ in outs)
    return pl.pallas_call(
        body,
        grid=grid,
        in_specs=[s for _, s in ins],
        out_specs=[s for _, _, s in outs],
        out_shape=[jax.ShapeDtypeStruct(s, d) for s, d, _ in outs],
        scratch_shapes=list(scratch),
        compiler_params=pltpu.CompilerParams(dimension_semantics=("arbitrary",) * len(grid), vmem_limit_bytes=VMEM),
        cost_estimate=pl.CostEstimate(flops=flops, transcendentals=0, bytes_accessed=moved),
        name=name,
    )(*(a for a, _ in ins))


def _qkv_body(h_ref, cos_ref, sin_ref, wq, wk, wv, a_ref, q_ref, k_ref, v_ref):
    wide = h_ref[...].astype(F32)
    a = _low(wide * _scale(wide))
    a_ref[...] = a
    cos, sin = cos_ref[...], sin_ref[...]
    for w, out, turned in ((wq, q_ref, True), (wk, k_ref, True), (wv, v_ref, False)):
        for at in range(0, w.shape[1], HEAD):
            y = _low(_nn(a, w[:, at : at + HEAD]))
            out[:, at : at + HEAD] = _low(_turn(y.astype(F32), cos, sin)) if turned else y


def fwd_qkv(h, cos, sin, wq, wk, wv):
    s, d = h.shape
    n = wq[2]
    blk = lambda c: _rows((ROWS, c))
    return _call(_qkv_body, (s // ROWS,), [(h, blk(d)), (cos, blk(HALF)), (sin, blk(HALF))] + [(w[0], _held(w)) for w in (wq, wk, wv)],
                 [((s, d), BF, blk(d))] + [((s, n), BF, blk(n))] * 3, 6 * s * d * n, name="qkv")


def _attn_body(q_ref, k_ref, v_ref, o_ref, lse_ref, top_s, mix_s, *, scale, bq, bk, heads):
    iq = pl.program_id(0)
    e = scale * LOG2E
    for i in range(heads):
        top_s[i : i + 1, :] = jnp.full((1, bq), NEG, F32)
        mix_s[i] = jnp.zeros((HEAD + 8, bq), F32)
    ones = jnp.ones((8, bk), BF)

    def block(first, lo, diagonal):
        here = pl.ds(first, bk)
        spans = [(lo, bk, True)] + ([(lo + bk, bq - lo - bk, False)] if lo + bk < bq else []) if diagonal else [(0, bq, False)]
        pieces = [(i, *span) for i in range(heads) for span in spans]
        scores = [_nt(k_ref[here, i * HEAD : (i + 1) * HEAD], q_ref[at : at + n, i * HEAD : (i + 1) * HEAD]) for i, at, n, _ in pieces]
        weights, keeps = [], []
        for (i, at, n, masked), s in zip(pieces, scores):
            if masked:
                ok = lax.broadcasted_iota(jnp.int32, (bk, n), 1) >= lax.broadcasted_iota(jnp.int32, (bk, n), 0)
                s = jnp.where(ok, s, HIDDEN)
            old = top_s[i : i + 1, at : at + n]
            top = jnp.maximum(old, s.max(axis=0, keepdims=True))
            top_s[i : i + 1, at : at + n] = top
            weights.append(_low(jnp.exp2((s - top) * e)))
            keeps.append(jnp.exp2((old - top) * e))
        for (i, at, n, _), p, keep in zip(pieces, weights, keeps):
            values = jnp.concatenate([v_ref[here, i * HEAD : (i + 1) * HEAD].T, ones], axis=0)
            mix_s[i, :, at : at + n] = mix_s[i, :, at : at + n] * keep + _nn(values, p)

    lax.fori_loop(0, iq * (bq // bk), lambda j, _: block(pl.multiple_of(j * bk, bk), 0, False), None)
    for t in range(bq // bk):
        block(pl.multiple_of(iq * bq + t * bk, bk), t * bk, True)
    for i in range(heads):
        top, total = top_s[i : i + 1, :], mix_s[i, HEAD : HEAD + 1, :]
        o_ref[:, i * HEAD : (i + 1) * HEAD] = _low((mix_s[i, :HEAD, :] * (1 / total)).T)
        lse_ref[i : i + 1, :] = top * scale + jnp.log(total)


FWD_BQ, FWD_BK = 1024, 512
BWD_BQ, BWD_BK = 1024, 256


def attend(q, k, v):
    s, n = q.shape
    heads, bq, bk = n // HEAD, FWD_BQ, FWD_BK
    whole = pl.BlockSpec((s, n), lambda i: (0, 0), pipeline_mode=pl.Buffered(1))
    return _call(functools.partial(_attn_body, scale=HEAD**-0.5, bq=bq, bk=bk, heads=heads), (s // bq,),
                 [(q, _rows((bq, n))), (k, whole), (v, whole)],
                 [((s, n), BF, _rows((bq, n))), ((heads, s), F32, pl.BlockSpec((heads, bq), lambda i: (0, i)))], 4 * s * s * n,
                 [pltpu.VMEM((heads, bq), F32), pltpu.VMEM((heads, HEAD + 8, bq), F32)], name="attend")


def _out_body(o_ref, h_ref, wo, h2_ref, b_ref):
    h2 = _low(h_ref[...].astype(F32) + _round(_nn(o_ref[...], wo[...])))
    h2_ref[...] = h2
    wide = h2.astype(F32)
    b_ref[...] = _low(wide * _scale(wide))


def fwd_out(o, h, wo):
    s, d = h.shape
    n = o.shape[1]
    return _call(_out_body, (s // ROWS,), [(o, _rows((ROWS, n))), (h, _rows((ROWS, d))), (wo[0], _held(wo))],
                 [((s, d), BF, _rows((ROWS, d)))] * 2, 2 * s * d * n, name="out")


def _gate_up_body(b_ref, wg, wu, act_ref, by_up_ref, by_gate_ref):
    here = pl.ds(pl.multiple_of(pl.program_id(1) * WIDE, WIDE), WIDE)
    b = b_ref[...]
    gate, up = _nn(b, wg[:, here]), _nn(b, wu[:, here])
    sig = jax.nn.sigmoid(gate)
    silu = gate * sig
    act_ref[...] = _low(silu * up)
    by_up_ref[...] = silu
    by_gate_ref[...] = up * (sig + silu * (1 - sig))


def fwd_gate_up(b, wg, wu):
    s, d = b.shape
    f = wg[2]
    blk = pl.BlockSpec((ROWS, WIDE), lambda i, j: (i, j))
    return _call(_gate_up_body, (s // ROWS, f // WIDE), [(b, _rows((ROWS, d))), (wg[0], _held(wg)), (wu[0], _held(wu))],
                 [((s, f), BF, blk), ((s, f), F32, blk), ((s, f), F32, blk)], 4 * s * d * f, name="gate_up")


def _down_body(act_ref, h_ref, wd, out_ref, *, parts, cut, n):
    total = None
    for j in range(parts):
        act = jnp.concatenate([act_ref[:, (i * parts + j) * cut : (i * parts + j + 1) * cut] for i in range(wd.shape[0] // cut)], axis=1)
        term = _nn(act, wd[:, j * n : (j + 1) * n])
        total = term if total is None else total + term
    out_ref[...] = _low(h_ref[...].astype(F32) + _round(total))


def fwd_down(act, h2, wd, cut):
    s, d = h2.shape
    f = act.shape[1]
    return _call(functools.partial(_down_body, parts=wd[2] // d, cut=cut, n=d), (s // ROWS,),
                 [(act, _rows((ROWS, f))), (h2, _rows((ROWS, d))), (wd[0], _held(wd))],
                 [((s, d), BF, _rows((ROWS, d)))], 2 * s * d * f, name="down")[0]


def _units_back_body(dy_ref, b_ref, by_up_ref, by_gate_ref, wd, dg_ref, du_ref, out_ref, b_s, *, rows):
    @pl.when(pl.program_id(0) == 0)
    def _():
        b_s[...] = b_ref[...].T

    n, wide = dy_ref.shape[1], dg_ref.shape[1]
    w = jnp.concatenate([wd[:, j * n : (j + 1) * n] for j in range(wd.shape[1] // n)], axis=0)
    for at in range(0, dy_ref.shape[0], rows):
        here = slice(at, at + rows)
        dact = _round(_nt(dy_ref[here, :], w))
        dg_ref[here, :] = _low(dact * by_gate_ref[here, :])
        du_ref[here, :] = _low(dact * by_up_ref[here, :])
    out_ref[:, :wide] = _low(_nn(b_s[...], dg_ref[...]))
    out_ref[:, wide:] = _low(_nn(b_s[...], du_ref[...]))


def units_back(dy, b, by_up, by_gate, wd, cut, wide, rows=512):
    s, d = dy.shape
    f = by_up.shape[1]
    array, _, columns, at = wd
    held = pl.BlockSpec((s, d), lambda j: (0, 0), pipeline_mode=pl.Buffered(1))
    blk = pl.BlockSpec((s, wide), lambda j: (0, j))
    return _call(functools.partial(_units_back_body, rows=rows), (f // wide,),
                 [(dy, held), (b, held), (by_up, blk), (by_gate, blk), (array, pl.BlockSpec((cut, columns), lambda j: (j, at)))],
                 [((s, f), BF, blk), ((s, f), BF, blk), ((d, 2 * f), BF, pl.BlockSpec((d, 2 * wide), lambda j: (0, j)))],
                 6 * s * d * f, [pltpu.VMEM((d, s), BF)], name="units_back")


def _mlp_back_body(dg_ref, du_ref, dy_ref, h2_ref, o_ref, wg, wu, wo, dh_ref, do_ref, delta_ref):
    by_b = _round(_round(_nt(dg_ref[...], wg[...])) + _round(_nt(du_ref[...], wu[...])))
    dh = _low(dy_ref[...].astype(F32) + _round(_norm_back(by_b, h2_ref[...].astype(F32))))
    dh_ref[...] = dh
    do = _low(_nt(dh, wo[...]))
    do_ref[...] = do
    both = do.astype(F32) * o_ref[...].astype(F32)
    for i in range(both.shape[1] // HEAD):
        delta_ref[i : i + 1, :] = jnp.sum(both[:, i * HEAD : (i + 1) * HEAD].T, axis=0, keepdims=True)


def mlp_back(dg, du, dy, h2, o, wg, wu, wo, rows=512):
    s, d = dy.shape
    f, n = dg.shape[1], o.shape[1]
    row = lambda c: _rows((rows, c))
    return _call(_mlp_back_body, (s // rows,),
                 [(dg, row(f)), (du, row(f)), (dy, row(d)), (h2, row(d)), (o, row(n))] + [(w[0], _held(w)) for w in (wg, wu, wo)],
                 [((s, d), BF, row(d)), ((s, n), BF, row(n)), ((n // HEAD, s), F32, pl.BlockSpec((n // HEAD, rows), lambda i: (0, i)))],
                 4 * s * d * f + 2 * s * d * n, name="mlp_back")


def _attn_back_body(q_ref, k_ref, v_ref, do_ref, lse_ref, delta_ref, cosq_ref, sinq_ref, cos_ref, sin_ref, dq_ref, dk_ref, dv_ref,
                    dq_s, dk_s, dv_s, *, scale, bq, bk, heads):
    iq = pl.program_id(1)
    e = scale * LOG2E

    @pl.when(iq == 0)
    def _():
        dk_s[...] = jnp.zeros_like(dk_s)
        dv_s[...] = jnp.zeros_like(dv_s)

    dq_s[...] = jnp.zeros_like(dq_s)
    lses = [lse_ref[0, i : i + 1, :] * LOG2E for i in range(heads)]
    deltas = [delta_ref[0, i : i + 1, :] for i in range(heads)]

    def block(first, lo, diagonal):
        here = pl.ds(first, bk)
        spans = [(lo, bk, True)] + ([(lo + bk, bq - lo - bk, False)] if lo + bk < bq else []) if diagonal else [(0, bq, False)]
        pieces = [(i, *span) for i in range(heads) for span in spans]
        col = lambda i: slice(i * HEAD, (i + 1) * HEAD)
        qs = [q_ref[at : at + n, col(i)] for i, at, n, _ in pieces]
        dos = [do_ref[at : at + n, col(i)] for i, at, n, _ in pieces]
        scores = [_nt(k_ref[here, col(p[0])], x) for p, x in zip(pieces, qs)]
        dps = [_nt(v_ref[here, col(p[0])], x) for p, x in zip(pieces, dos)]
        for m, (i, at, n, masked) in enumerate(pieces):
            p = jnp.exp2(scores[m] * e - lses[i][:, at : at + n])
            if masked:
                ok = lax.broadcasted_iota(jnp.int32, (bk, n), 1) >= lax.broadcasted_iota(jnp.int32, (bk, n), 0)
                p = jnp.where(ok, p, 0.0)
            ds = _low(p * (dps[m] - deltas[i][:, at : at + n]))
            dv_s[here, col(i)] += _nn(_low(p), dos[m])
            dk_s[here, col(i)] += _nn(ds, qs[m])
            dq_s[i, :, at : at + n] += _nn(k_ref[here, col(i)].T, ds)

    lax.fori_loop(0, iq * (bq // bk), lambda j, _: block(pl.multiple_of(j * bk, bk), 0, False), None)
    for t in range(bq // bk):
        block(pl.multiple_of(iq * bq + t * bk, bk), t * bk, True)
    for i in range(heads):
        dq_ref[:, i * HEAD : (i + 1) * HEAD] = _low(_turn(_round((dq_s[i] * scale).T), cosq_ref[...], -sinq_ref[...]))

    @pl.when(iq == pl.num_programs(1) - 1)
    def _():
        for i in range(heads):
            dk_ref[:, i * HEAD : (i + 1) * HEAD] = _low(_turn(_round(dk_s[:, i * HEAD : (i + 1) * HEAD] * scale), cos_ref[...], -sin_ref[...]))
            dv_ref[:, i * HEAD : (i + 1) * HEAD] = _low(dv_s[:, i * HEAD : (i + 1) * HEAD])


def attend_back(q, k, v, do, lse, delta, cos, sin):
    s, n = q.shape
    kb, bq, bk = 2, BWD_BQ, BWD_BK
    w, groups = kb * HEAD, n // HEAD // kb
    part = pl.BlockSpec((bq, w), lambda g, i: (i, g))
    whole = pl.BlockSpec((s, w), lambda g, i: (0, g))
    stats = pl.BlockSpec((1, kb, bq), lambda g, i: (g, 0, i))
    table = pl.BlockSpec((s, HALF), lambda g, i: (0, 0), pipeline_mode=pl.Buffered(1))
    near = pl.BlockSpec((bq, HALF), lambda g, i: (i, 0))
    return _call(functools.partial(_attn_back_body, scale=HEAD**-0.5, bq=bq, bk=bk, heads=kb), (groups, s // bq),
                 [(q, part), (k, whole), (v, whole), (do, part), (lse.reshape(groups, kb, s), stats), (delta.reshape(groups, kb, s), stats),
                  (cos, near), (sin, near), (cos, table), (sin, table)],
                 [((s, n), BF, part), ((s, n), BF, whole), ((s, n), BF, whole)], 5 * s * s * n,
                 [pltpu.VMEM((kb, HEAD, bq), F32), pltpu.VMEM((s, w), F32), pltpu.VMEM((s, w), F32)], name="attend_back")


def _qkv_back_body(dq_ref, dk_ref, dv_ref, h_ref, dh_ref, wq, wk, wv, out_ref):
    by_a = _round(_nt(dq_ref[...], wq[...])) + _round(_nt(dk_ref[...], wk[...]))
    by_a = _round(_round(by_a) + _round(_nt(dv_ref[...], wv[...])))
    out_ref[...] = _low(dh_ref[...].astype(F32) + _round(_norm_back(by_a, h_ref[...].astype(F32))))


def qkv_back(dq, dk, dv, h, dh, wq, wk, wv):
    s, d = h.shape
    n = dq.shape[1]
    return _call(_qkv_back_body, (s // ROWS,), [(x, _rows((ROWS, x.shape[1]))) for x in (dq, dk, dv, h, dh)] + [(w[0], _held(w)) for w in (wq, wk, wv)],
                 [((s, d), BF, _rows((ROWS, d)))], 6 * s * d * n, name="qkv_back")[0]


def _weight_back_body(*refs, plan, per):
    count = len(plan)
    a_refs, b_refs, out_ref, a_s = refs[: max(plan) + 1], refs[-count - 2 : -2], refs[-2], refs[-1]
    j = pl.program_id(0)
    for i, which in enumerate(plan):
        if i == 0 or plan[i - 1] != which:
            @pl.when(j == i * per)
            def _():
                a_s[...] = a_refs[which][...].T

        @pl.when((j >= i * per) & (j < (i + 1) * per))
        def _():
            out_ref[...] = _low(_nn(a_s[...], b_refs[i][...]))


def weight_back(pairs, wide=512):
    firsts, plan = [], []
    for a, _ in pairs:
        if not any(a is x for x in firsts):
            firsts.append(a)
        plan.append([a is x for x in firsts].index(True))
    bs = [b for _, b in pairs]
    (s, m), n = firsts[0].shape, bs[0].shape[1]
    per = n // wide
    spec = lambda i: pl.BlockSpec((s, wide), lambda j: (0, jnp.clip(j - i * per, 0, per - 1)))
    return _call(functools.partial(_weight_back_body, plan=plan, per=per), (per * len(bs),),
                 [(a, pl.BlockSpec((s, m), lambda j: (0, 0), pipeline_mode=pl.Buffered(1))) for a in firsts] + [(b, spec(i)) for i, b in enumerate(bs)],
                 [((m, n * len(bs)), BF, pl.BlockSpec((m, wide), lambda j: (0, j)))], 2 * s * m * n * len(bs), [pltpu.VMEM((m, s), BF)], name="weight_back")[0]


def _tall_back_body(a_ref, b_ref, out_ref, *, cut, n):
    res = _low(_nn(a_ref[...].T, b_ref[...]))
    for j in range(res.shape[0] // cut):
        out_ref[:, j * n : (j + 1) * n] = res[j * cut : (j + 1) * cut, :]


def tall_back(a, b, cut, tall):
    (s, m), n = a.shape, b.shape[1]
    rows, columns = m * cut // tall, n * tall // cut
    return _call(functools.partial(_tall_back_body, cut=cut, n=n), (m // tall,),
                 [(a, pl.BlockSpec((s, tall), lambda j: (0, j))), (b, pl.BlockSpec((s, n), lambda j: (0, 0), pipeline_mode=pl.Buffered(1)))],
                 [((rows, columns), BF, pl.BlockSpec((cut, columns), lambda j: (j, 0)))], 2 * s * m * n, name="tall_back")[0]


def _pack_body(*refs, plan):
    count = sum(len(p) for p in plan)
    ins, outs = refs[:count], refs[count:]
    at = 0
    for out, parts in zip(outs, plan):
        column = 0
        for _ in parts:
            ref = ins[at]
            at += 1
            rows, n = out.shape[0], ref.shape[2]
            for j in range(ref.shape[1] // rows):
                out[:, column : column + n] = ref[0, j * rows : (j + 1) * rows, :]
                column += n


def packed(plan, cut):
    flat = [p for parts in plan for p in parts]
    ins = [(w, pl.BlockSpec((1, *w.shape[1:]), lambda i, at=layer: (at, 0, 0))) for w, layer in flat]
    wide = [sum(w.shape[1] * w.shape[2] // cut for w, _ in parts) for parts in plan]
    return _call(functools.partial(_pack_body, plan=plan), (1,), ins,
                 [((cut, n), BF, pl.BlockSpec((cut, n), lambda i: (0, 0))) for n in wide], 0, name="pack")


def squares(g, so_far):
    tile = pl.BlockSpec((8, 128), lambda i: (0, 0))
    wide = min(g.shape[1], 2048)
    return _call(_squares_grid_body, (g.shape[1] // wide,), [(g, pl.BlockSpec((g.shape[0], wide), lambda i: (0, i))), (so_far, tile)],
                 [((8, 128), F32, tile)], 2 * g.size, name="squares")[0]


def _squares_grid_body(g_ref, so_far_ref, out_ref):
    @pl.when(pl.program_id(0) == 0)
    def _():
        out_ref[...] = so_far_ref[...]

    total = out_ref[...]
    for r in range(0, g_ref.shape[0], 16):
        g = g_ref[r : r + 16, :].astype(F32)
        g = g * g
        row = g[:8] + g[8:]
        parts = [row[:, c : c + 128] for c in range(0, row.shape[1], 128)]
        while len(parts) > 1:
            parts = [x + y for x, y in zip(parts[::2], parts[1::2])]
        total = total + parts[0]
    out_ref[...] = total


def _factor_body(own_ref, out_ref, held, send_sem, recv_sem, *, n, count):
    rep, me = lax.axis_index("rep"), lax.axis_index("dp")
    others = [(rep, lax.rem(me + k, n)) for k in range(1, n)]
    barrier = pltpu.get_barrier_semaphore()
    for other in others:
        pl.semaphore_signal(barrier, inc=1, device_id=other, device_id_type=pl.DeviceIdType.MESH)
    pl.semaphore_wait(barrier, n - 1)
    copies = [pltpu.make_async_remote_copy(src_ref=own_ref, dst_ref=held.at[k], send_sem=send_sem.at[k], recv_sem=recv_sem.at[k],
                                           device_id=other, device_id_type=pl.DeviceIdType.MESH) for k, other in enumerate(others)]
    for copy in copies:
        copy.start()
    for copy in copies:
        copy.wait()
    total = own_ref[...]
    for k in range(n - 1):
        total = total + held[k]
    total = jnp.sum(jnp.sum(total, axis=0, keepdims=True), axis=1, keepdims=True)
    out_ref[...] = jnp.broadcast_to(jnp.minimum(1.0, 0.5 * lax.rsqrt(total / count + 1e-30)), out_ref.shape)


def clip_factor(own, n, count):
    return pl.pallas_call(
        functools.partial(_factor_body, n=n, count=count),
        out_shape=jax.ShapeDtypeStruct((8, 128), F32),
        in_specs=[pl.BlockSpec(memory_space=pltpu.VMEM)],
        out_specs=pl.BlockSpec(memory_space=pltpu.VMEM),
        scratch_shapes=[pltpu.VMEM((n - 1, 8, 128), F32), pltpu.SemaphoreType.DMA((n - 1,)), pltpu.SemaphoreType.DMA((n - 1,))],
        compiler_params=pltpu.CompilerParams(collective_id=0, has_side_effects=True),
        cost_estimate=pl.CostEstimate(flops=10**6, transcendentals=0, bytes_accessed=65536),
        name="clip_factor",
    )(own)


def _adamw_body(*refs, n, f, tall):
    factor_ref, sums, rest = refs[0], refs[1:7], refs[7:]
    ins, outs = rest[:21], rest[21:]
    first = pl.program_id(0) == 0
    factor = factor_ref[0:1, 0:1]
    g_of = lambda i, columns: jnp.where(first, sums[i][:, columns], sums[3 + i][:, columns]).astype(F32)
    pieces = lambda k: [slice(at + k * tall, at + (k + 1) * tall) for at in range(0, 2 * f, 2 * tall)]
    where = [(0, [slice(i * n, (i + 1) * n)]) for i in range(4)] + [(1, pieces(0)), (1, pieces(1)), (2, [slice(None)])]
    for i, (which, columns) in enumerate(where):
        w, m, v = (ins[i + 7 * k][0].astype(F32) for k in range(3))
        g = jnp.concatenate([g_of(which, piece) for piece in columns], axis=1) * factor
        m = 0.9 * m + 0.1 * g
        v = 0.95 * v + 0.05 * g * g
        outs[i][0] = _low(w - 0.02 * (m * lax.rsqrt(v + 1e-8) + 0.1 * w))
        outs[7 + i][0] = m
        outs[14 + i][0] = v


def adamw(factor, sums, weights, m, v):
    n, f = weights[0].shape[2], weights[4].shape[2]
    cut, tall = weights[0].shape[1], weights[6].shape[1]
    steps = 8
    per, half = tall // steps, cut * steps // tall

    def block(a):
        return pl.BlockSpec((1, a.shape[1] // steps, a.shape[2]), lambda l, t: (l, t, 0))

    def held(layer, i, a):
        at = lambda l, t: jnp.where(l == layer, t, (1 - layer) * (steps - 1))
        if i == 2:
            return pl.BlockSpec((per, n), lambda l, t: (lax.rem(at(l, t), half), lax.div(at(l, t), half)))
        return pl.BlockSpec((a.shape[0] // steps, a.shape[1]), lambda l, t: (at(l, t), 0))

    arrays = (*weights, *m, *v)
    ins = [(factor, pl.BlockSpec((8, 128), lambda l, t: (0, 0)))]
    ins += [(a, held(layer, i, a)) for layer in range(2) for i, a in enumerate(sums[layer])]
    ins += [(a, block(a)) for a in arrays]
    return _call(functools.partial(_adamw_body, n=n, f=f, tall=tall), (2, steps), ins, [(a.shape, a.dtype, block(a)) for a in arrays], 10**8, name="adamw")


def solution(mesh):
    def gathered(w):
        return lax.all_gather(w, "dp", axis=0, tiled=True)

    def scattered(g):
        return lax.psum_scatter(g, "dp", scatter_dimension=0, tiled=True)

    def step(x, dy, *arrays):
        weights, m, v = (arrays[i : i + 7] for i in (0, 7, 14))
        s, d = x.shape[1:]
        n, f = weights[0].shape[2], weights[4].shape[2]
        cut, tall = weights[0].shape[1], weights[6].shape[1]
        tie = lambda *xs: lax.optimization_barrier(xs)

        (p0,) = packed([[(weights[i], 0) for i in range(4)]], cut)
        rest = packed([[(weights[4], 0), (weights[5], 0)], [(weights[6], 0)] + [(weights[i], 1) for i in range(4)],
                       [(weights[4], 1), (weights[5], 1)], [(weights[6], 1)]], cut)
        w0, w1, w2, w3, w4 = (gathered(p) for p in (p0, *rest))
        full = [dict(w_gate=(gu, d, f, 0), w_up=(gu, d, f, 1), w_down=(down, d, f, 0),
                     **{name: (qkvo, d, n, first + i) for i, name in enumerate(NAMES[:4])})
                for gu, down, qkvo, first in ((w1, w2, w0, 0), (w3, w4, w2, 4))]

        angle = jnp.arange(s, dtype=F32)[:, None] * THETA ** (-jnp.arange(HALF, dtype=F32) / HALF)
        cos, sin = jnp.cos(angle), jnp.sin(angle)

        h, kept = x[0], []
        for w in full:
            a, q, k, vv = fwd_qkv(h, cos, sin, w["wq"], w["wk"], w["wv"])
            o, lse = attend(q, k, vv)
            h2, b = fwd_out(o, h, w["wo"])
            act, by_up, by_gate = fwd_gate_up(b, w["w_gate"], w["w_up"])
            kept.append((h, a, q, k, vv, o, lse, h2, b, act, by_up, by_gate))
            if w is not full[-1]:
                h = fwd_down(act, h2, w["w_down"], cut)

        by_h = dy[0]
        for number in (1, 0):
            w = full[number]
            h, a, q, k, vv, o, lse, h2, b, act, by_up, by_gate = kept[number]
            g_down = tall_back(act, by_h, cut, tall)
            g_down, by_h = tie(g_down, by_h)
            s_down = scattered(g_down)
            if number == 0:
                s_gu1, by_up = tie(s_gu, by_up)
            dg, du, g_gu = units_back(by_h, b, by_up, by_gate, w["w_down"], cut, tall)
            if number == 0:
                s_qkvo1, g_gu, dg = tie(s_qkvo, g_gu, dg)
            else:
                g_gu, dg = tie(g_gu, dg)
            s_gu = scattered(g_gu)
            dh, do, delta = mlp_back(dg, du, by_h, h2, o, w["w_gate"], w["w_up"], w["wo"])
            dq, dk, dv = attend_back(q, k, vv, do, lse, delta, cos, sin)
            s_down, dq = tie(s_down, dq)
            g_qkvo = weight_back([(a, dq), (a, dk), (a, dv), (o, dh)])
            if number:
                g_qkvo, dq = tie(g_qkvo, dq)
                s_down1 = s_down
                by_h = qkv_back(dq, dk, dv, h, dh, w["wq"], w["wk"], w["wv"])
            else:
                s_gu, g_qkvo = tie(s_gu, g_qkvo)
            s_qkvo = scattered(g_qkvo)
        sums = ((s_qkvo, s_gu, s_down), (s_qkvo1, s_gu1, s_down1))
        total = jnp.zeros((8, 128), F32)
        for g in (s_down1, s_gu1, s_qkvo1, s_down, s_gu, s_qkvo):
            total = squares(g, total)
        size = mesh.shape["dp"]
        factor = clip_factor(total, size, float(size * sum(g.size for layer in sums for g in layer)))
        return tuple(adamw(factor, sums, weights, m, v))

    states, rows = P(("rep", "dp"), None, None), P(None, "dp", None)
    return jax.shard_map(
        step,
        mesh=mesh,
        in_specs=(states, states) + (rows,) * 21,
        out_specs=(P("rep", "dp", None),) * 21,
        check_vma=False,
    )
```

```python
import functools

import jax
import jax.numpy as jnp
from jax import lax
from jax.experimental import pallas as pl
from jax.experimental.pallas import tpu as pltpu
from jax.sharding import PartitionSpec as P

NEG = -1e30
HIDDEN = 2 * NEG
LOG2E = 1.4426950408889634
VMEM = 62 * 2**20
HEAD = 256
HALF = HEAD // 2
THETA = 10000
NAMES = ("wq", "wk", "wv", "wo", "w_gate", "w_up", "w_down")
BF, F32 = jnp.bfloat16, jnp.float32
ROWS = 512
WIDE = 1024


def _nn(a, b):
    return lax.dot_general(a, b, (((1,), (0,)), ((), ())), preferred_element_type=F32)


def _nt(a, b):
    return lax.dot_general(a, b, (((1,), (1,)), ((), ())), preferred_element_type=F32)


def _low(x):
    return x.astype(BF)


def _round(x):
    return x.astype(BF).astype(F32)


def _scale(wide):
    return lax.rsqrt(jnp.mean(wide * wide, -1, keepdims=True) + 1e-6)


def _norm_back(by_b, wide):
    scale = _scale(wide)
    by_scale = jnp.sum(by_b * wide, -1, keepdims=True)
    return by_b * scale - wide * (scale * scale * scale * by_scale * (1 / wide.shape[-1]))


def _turn(t, cos, sin):
    a, b = t[:, :HALF], t[:, HALF:]
    return jnp.concatenate([a * cos - b * sin, b * cos + a * sin], -1)


def _rows(shape):
    return pl.BlockSpec(shape, lambda i, *_: (i, 0))


def _held(w):
    _, rows, columns, at = w
    return pl.BlockSpec((rows, columns), lambda *_: (0, at), pipeline_mode=pl.Buffered(1))


def _call(body, grid, ins, outs, flops, scratch=(), name=None, order=None):
    size = lambda s, d: int(jnp.dtype(d).itemsize) * functools.reduce(lambda a, b: a * b, s, 1)
    moved = sum(size(a.shape, a.dtype) for a, _ in ins) + sum(size(s, d) for s, d, _ in outs)
    return pl.pallas_call(
        body,
        grid=grid,
        in_specs=[s for _, s in ins],
        out_specs=[s for _, _, s in outs],
        out_shape=[jax.ShapeDtypeStruct(s, d) for s, d, _ in outs],
        scratch_shapes=list(scratch),
        compiler_params=pltpu.CompilerParams(dimension_semantics=("arbitrary",) * len(grid), vmem_limit_bytes=VMEM),
        cost_estimate=pl.CostEstimate(flops=flops, transcendentals=0, bytes_accessed=moved),
        name=name,
    )(*(a for a, _ in ins))


def _qkv_body(h_ref, cos_ref, sin_ref, wq, wk, wv, a_ref, q_ref, k_ref, v_ref):
    wide = h_ref[...].astype(F32)
    a = _low(wide * _scale(wide))
    a_ref[...] = a
    cos, sin = cos_ref[...], sin_ref[...]
    for w, out, turned in ((wq, q_ref, True), (wk, k_ref, True), (wv, v_ref, False)):
        for at in range(0, w.shape[1], HEAD):
            y = _low(_nn(a, w[:, at : at + HEAD]))
            out[:, at : at + HEAD] = _low(_turn(y.astype(F32), cos, sin)) if turned else y


def fwd_qkv(h, cos, sin, wq, wk, wv):
    s, d = h.shape
    n = wq[2]
    blk = lambda c: _rows((ROWS, c))
    return _call(_qkv_body, (s // ROWS,), [(h, blk(d)), (cos, blk(HALF)), (sin, blk(HALF))] + [(w[0], _held(w)) for w in (wq, wk, wv)],
                 [((s, d), BF, blk(d))] + [((s, n), BF, blk(n))] * 3, 6 * s * d * n, name="qkv")


def _attn_body(q_ref, k_ref, v_ref, o_ref, lse_ref, top_s, mix_s, *, scale, bq, bk, heads):
    iq = pl.program_id(0)
    e = scale * LOG2E
    for i in range(heads):
        top_s[i : i + 1, :] = jnp.full((1, bq), NEG, F32)
        mix_s[i] = jnp.zeros((HEAD + 8, bq), F32)
    ones = jnp.ones((8, bk), BF)

    def block(first, lo, diagonal):
        here = pl.ds(first, bk)
        spans = [(lo, bk, True)] + ([(lo + bk, bq - lo - bk, False)] if lo + bk < bq else []) if diagonal else [(0, bq, False)]
        pieces = [(i, *span) for i in range(heads) for span in spans]
        scores = [_nt(k_ref[here, i * HEAD : (i + 1) * HEAD], q_ref[at : at + n, i * HEAD : (i + 1) * HEAD]) for i, at, n, _ in pieces]
        weights, keeps = [], []
        for (i, at, n, masked), s in zip(pieces, scores):
            if masked:
                ok = lax.broadcasted_iota(jnp.int32, (bk, n), 1) >= lax.broadcasted_iota(jnp.int32, (bk, n), 0)
                s = jnp.where(ok, s, HIDDEN)
            old = top_s[i : i + 1, at : at + n]
            top = jnp.maximum(old, s.max(axis=0, keepdims=True))
            top_s[i : i + 1, at : at + n] = top
            weights.append(_low(jnp.exp2((s - top) * e)))
            keeps.append(jnp.exp2((old - top) * e))
        for (i, at, n, _), p, keep in zip(pieces, weights, keeps):
            values = jnp.concatenate([v_ref[here, i * HEAD : (i + 1) * HEAD].T, ones], axis=0)
            mix_s[i, :, at : at + n] = mix_s[i, :, at : at + n] * keep + _nn(values, p)

    lax.fori_loop(0, iq * (bq // bk), lambda j, _: block(pl.multiple_of(j * bk, bk), 0, False), None)
    for t in range(bq // bk):
        block(pl.multiple_of(iq * bq + t * bk, bk), t * bk, True)
    for i in range(heads):
        top, total = top_s[i : i + 1, :], mix_s[i, HEAD : HEAD + 1, :]
        o_ref[:, i * HEAD : (i + 1) * HEAD] = _low((mix_s[i, :HEAD, :] * (1 / total)).T)
        lse_ref[i : i + 1, :] = top * scale + jnp.log(total)


FWD_BQ, FWD_BK = 1024, 512
BWD_BQ, BWD_BK = 1024, 256


def attend(q, k, v):
    s, n = q.shape
    heads, bq, bk = n // HEAD, FWD_BQ, FWD_BK
    whole = pl.BlockSpec((s, n), lambda i: (0, 0), pipeline_mode=pl.Buffered(1))
    return _call(functools.partial(_attn_body, scale=HEAD**-0.5, bq=bq, bk=bk, heads=heads), (s // bq,),
                 [(q, _rows((bq, n))), (k, whole), (v, whole)],
                 [((s, n), BF, _rows((bq, n))), ((heads, s), F32, pl.BlockSpec((heads, bq), lambda i: (0, i)))], 4 * s * s * n,
                 [pltpu.VMEM((heads, bq), F32), pltpu.VMEM((heads, HEAD + 8, bq), F32)], name="attend")


def _out_body(o_ref, h_ref, wo, h2_ref, b_ref):
    h2 = _low(h_ref[...].astype(F32) + _round(_nn(o_ref[...], wo[...])))
    h2_ref[...] = h2
    wide = h2.astype(F32)
    b_ref[...] = _low(wide * _scale(wide))


def fwd_out(o, h, wo):
    s, d = h.shape
    n = o.shape[1]
    return _call(_out_body, (s // ROWS,), [(o, _rows((ROWS, n))), (h, _rows((ROWS, d))), (wo[0], _held(wo))],
                 [((s, d), BF, _rows((ROWS, d)))] * 2, 2 * s * d * n, name="out")


def _gate_up_body(b_ref, wg, wu, act_ref, by_up_ref, by_gate_ref):
    here = pl.ds(pl.multiple_of(pl.program_id(1) * WIDE, WIDE), WIDE)
    b = b_ref[...]
    gate, up = _nn(b, wg[:, here]), _nn(b, wu[:, here])
    sig = jax.nn.sigmoid(gate)
    silu = gate * sig
    act_ref[...] = _low(silu * up)
    by_up_ref[...] = silu
    by_gate_ref[...] = up * (sig + silu * (1 - sig))


def fwd_gate_up(b, wg, wu):
    s, d = b.shape
    f = wg[2]
    blk = pl.BlockSpec((ROWS, WIDE), lambda i, j: (i, j))
    return _call(_gate_up_body, (s // ROWS, f // WIDE), [(b, _rows((ROWS, d))), (wg[0], _held(wg)), (wu[0], _held(wu))],
                 [((s, f), BF, blk), ((s, f), F32, blk), ((s, f), F32, blk)], 4 * s * d * f, name="gate_up")


def _down_body(act_ref, h_ref, wd, out_ref, *, parts, cut, n):
    total = None
    for j in range(parts):
        act = jnp.concatenate([act_ref[:, (i * parts + j) * cut : (i * parts + j + 1) * cut] for i in range(wd.shape[0] // cut)], axis=1)
        term = _nn(act, wd[:, j * n : (j + 1) * n])
        total = term if total is None else total + term
    out_ref[...] = _low(h_ref[...].astype(F32) + _round(total))


def fwd_down(act, h2, wd, cut):
    s, d = h2.shape
    f = act.shape[1]
    return _call(functools.partial(_down_body, parts=wd[2] // d, cut=cut, n=d), (s // ROWS,),
                 [(act, _rows((ROWS, f))), (h2, _rows((ROWS, d))), (wd[0], _held(wd))],
                 [((s, d), BF, _rows((ROWS, d)))], 2 * s * d * f, name="down")[0]


def _units_back_body(dy_ref, b_ref, by_up_ref, by_gate_ref, wd, dg_ref, du_ref, out_ref, b_s, *, rows):
    @pl.when(pl.program_id(0) == 0)
    def _():
        b_s[...] = b_ref[...].T

    n, wide = dy_ref.shape[1], dg_ref.shape[1]
    w = jnp.concatenate([wd[:, j * n : (j + 1) * n] for j in range(wd.shape[1] // n)], axis=0)
    for at in range(0, dy_ref.shape[0], rows):
        here = slice(at, at + rows)
        dact = _round(_nt(dy_ref[here, :], w))
        dg_ref[here, :] = _low(dact * by_gate_ref[here, :])
        du_ref[here, :] = _low(dact * by_up_ref[here, :])
    out_ref[:, :wide] = _low(_nn(b_s[...], dg_ref[...]))
    out_ref[:, wide:] = _low(_nn(b_s[...], du_ref[...]))


def units_back(dy, b, by_up, by_gate, wd, cut, wide, rows=512):
    s, d = dy.shape
    f = by_up.shape[1]
    array, _, columns, at = wd
    held = pl.BlockSpec((s, d), lambda j: (0, 0), pipeline_mode=pl.Buffered(1))
    blk = pl.BlockSpec((s, wide), lambda j: (0, j))
    return _call(functools.partial(_units_back_body, rows=rows), (f // wide,),
                 [(dy, held), (b, held), (by_up, blk), (by_gate, blk), (array, pl.BlockSpec((cut, columns), lambda j: (j, at)))],
                 [((s, f), BF, blk), ((s, f), BF, blk), ((d, 2 * f), BF, pl.BlockSpec((d, 2 * wide), lambda j: (0, j)))],
                 6 * s * d * f, [pltpu.VMEM((d, s), BF)], name="units_back")


def _mlp_back_body(dg_ref, du_ref, dy_ref, h2_ref, o_ref, wg, wu, wo, dh_ref, do_ref, delta_ref):
    by_b = _round(_round(_nt(dg_ref[...], wg[...])) + _round(_nt(du_ref[...], wu[...])))
    dh = _low(dy_ref[...].astype(F32) + _round(_norm_back(by_b, h2_ref[...].astype(F32))))
    dh_ref[...] = dh
    do = _low(_nt(dh, wo[...]))
    do_ref[...] = do
    both = do.astype(F32) * o_ref[...].astype(F32)
    for i in range(both.shape[1] // HEAD):
        delta_ref[i // 2, i % 2 : i % 2 + 1, :] = jnp.sum(both[:, i * HEAD : (i + 1) * HEAD].T, axis=0, keepdims=True)


def mlp_back(dg, du, dy, h2, o, wg, wu, wo, rows=512):
    s, d = dy.shape
    f, n = dg.shape[1], o.shape[1]
    row = lambda c: _rows((rows, c))
    return _call(_mlp_back_body, (s // rows,),
                 [(dg, row(f)), (du, row(f)), (dy, row(d)), (h2, row(d)), (o, row(n))] + [(w[0], _held(w)) for w in (wg, wu, wo)],
                 [((s, d), BF, row(d)), ((s, n), BF, row(n)), ((n // HEAD // 2, 2, s), F32, pl.BlockSpec((n // HEAD // 2, 2, rows), lambda i: (0, 0, i)))],
                 4 * s * d * f + 2 * s * d * n, name="mlp_back")


def _attn_back_body(q_ref, k_ref, v_ref, do_ref, lse_ref, delta_ref, cosq_ref, sinq_ref, cos_ref, sin_ref, dq_ref, dk_ref, dv_ref,
                    dq_s, dk_s, dv_s, *, scale, bq, bk, heads):
    iq = pl.program_id(1)
    e = scale * LOG2E

    @pl.when(iq == 0)
    def _():
        dk_s[...] = jnp.zeros_like(dk_s)
        dv_s[...] = jnp.zeros_like(dv_s)

    dq_s[...] = jnp.zeros_like(dq_s)
    lses = [lse_ref[0, i : i + 1, :] * LOG2E for i in range(heads)]
    deltas = [delta_ref[0, i : i + 1, :] for i in range(heads)]

    def block(first, lo, diagonal):
        here = pl.ds(first, bk)
        spans = [(lo, bk, True)] + ([(lo + bk, bq - lo - bk, False)] if lo + bk < bq else []) if diagonal else [(0, bq, False)]
        pieces = [(i, *span) for i in range(heads) for span in spans]
        col = lambda i: slice(i * HEAD, (i + 1) * HEAD)
        qs = [q_ref[at : at + n, col(i)] for i, at, n, _ in pieces]
        dos = [do_ref[at : at + n, col(i)] for i, at, n, _ in pieces]
        scores = [_nt(k_ref[here, col(p[0])], x) for p, x in zip(pieces, qs)]
        dps = [_nt(v_ref[here, col(p[0])], x) for p, x in zip(pieces, dos)]
        for m, (i, at, n, masked) in enumerate(pieces):
            p = jnp.exp2(scores[m] * e - lses[i][:, at : at + n])
            if masked:
                ok = lax.broadcasted_iota(jnp.int32, (bk, n), 1) >= lax.broadcasted_iota(jnp.int32, (bk, n), 0)
                p = jnp.where(ok, p, 0.0)
            ds = _low(p * (dps[m] - deltas[i][:, at : at + n]))
            dv_s[here, col(i)] += _nn(_low(p), dos[m])
            dk_s[here, col(i)] += _nn(ds, qs[m])
            dq_s[i, :, at : at + n] += _nn(k_ref[here, col(i)].T, ds)

    lax.fori_loop(0, iq * (bq // bk), lambda j, _: block(pl.multiple_of(j * bk, bk), 0, False), None)
    for t in range(bq // bk):
        block(pl.multiple_of(iq * bq + t * bk, bk), t * bk, True)
    for i in range(heads):
        dq_ref[:, i * HEAD : (i + 1) * HEAD] = _low(_turn(_round((dq_s[i] * scale).T), cosq_ref[...], -sinq_ref[...]))

    @pl.when(iq == pl.num_programs(1) - 1)
    def _():
        for i in range(heads):
            dk_ref[:, i * HEAD : (i + 1) * HEAD] = _low(_turn(_round(dk_s[:, i * HEAD : (i + 1) * HEAD] * scale), cos_ref[...], -sin_ref[...]))
            dv_ref[:, i * HEAD : (i + 1) * HEAD] = _low(dv_s[:, i * HEAD : (i + 1) * HEAD])


def attend_back(q, k, v, do, lse, delta, cos, sin):
    s, n = q.shape
    kb, bq, bk = 2, BWD_BQ, BWD_BK
    w, groups = kb * HEAD, n // HEAD // kb
    part = pl.BlockSpec((bq, w), lambda g, i: (i, g))
    whole = pl.BlockSpec((s, w), lambda g, i: (0, g))
    stats = pl.BlockSpec((1, kb, bq), lambda g, i: (g, 0, i))
    table = pl.BlockSpec((s, HALF), lambda g, i: (0, 0), pipeline_mode=pl.Buffered(1))
    near = pl.BlockSpec((bq, HALF), lambda g, i: (i, 0))
    return _call(functools.partial(_attn_back_body, scale=HEAD**-0.5, bq=bq, bk=bk, heads=kb), (groups, s // bq),
                 [(q, part), (k, whole), (v, whole), (do, part), (lse.reshape(groups, kb, s), stats), (delta.reshape(groups, kb, s), stats),
                  (cos, near), (sin, near), (cos, table), (sin, table)],
                 [((s, n), BF, part), ((s, n), BF, whole), ((s, n), BF, whole)], 5 * s * s * n,
                 [pltpu.VMEM((kb, HEAD, bq), F32), pltpu.VMEM((s, w), F32), pltpu.VMEM((s, w), F32)], name="attend_back")


def _qkv_back_body(dq_ref, dk_ref, dv_ref, h_ref, dh_ref, wq, wk, wv, out_ref):
    by_a = _round(_nt(dq_ref[...], wq[...])) + _round(_nt(dk_ref[...], wk[...]))
    by_a = _round(_round(by_a) + _round(_nt(dv_ref[...], wv[...])))
    out_ref[...] = _low(dh_ref[...].astype(F32) + _round(_norm_back(by_a, h_ref[...].astype(F32))))


def qkv_back(dq, dk, dv, h, dh, wq, wk, wv):
    s, d = h.shape
    n = dq.shape[1]
    return _call(_qkv_back_body, (s // ROWS,), [(x, _rows((ROWS, x.shape[1]))) for x in (dq, dk, dv, h, dh)] + [(w[0], _held(w)) for w in (wq, wk, wv)],
                 [((s, d), BF, _rows((ROWS, d)))], 6 * s * d * n, name="qkv_back")[0]


def _weight_back_body(*refs, plan, per):
    count = len(plan)
    a_refs, b_refs, out_ref, a_s = refs[: max(plan) + 1], refs[-count - 2 : -2], refs[-2], refs[-1]
    j = pl.program_id(0)
    for i, which in enumerate(plan):
        if i == 0 or plan[i - 1] != which:
            @pl.when(j == i * per)
            def _():
                a_s[...] = a_refs[which][...].T

        @pl.when((j >= i * per) & (j < (i + 1) * per))
        def _():
            out_ref[...] = _low(_nn(a_s[...], b_refs[i][...]))


def weight_back(pairs, wide=512):
    firsts, plan = [], []
    for a, _ in pairs:
        if not any(a is x for x in firsts):
            firsts.append(a)
        plan.append([a is x for x in firsts].index(True))
    bs = [b for _, b in pairs]
    (s, m), n = firsts[0].shape, bs[0].shape[1]
    per = n // wide
    spec = lambda i: pl.BlockSpec((s, wide), lambda j: (0, jnp.clip(j - i * per, 0, per - 1)))
    return _call(functools.partial(_weight_back_body, plan=plan, per=per), (per * len(bs),),
                 [(a, pl.BlockSpec((s, m), lambda j: (0, 0), pipeline_mode=pl.Buffered(1))) for a in firsts] + [(b, spec(i)) for i, b in enumerate(bs)],
                 [((m, n * len(bs)), BF, pl.BlockSpec((m, wide), lambda j: (0, j)))], 2 * s * m * n * len(bs), [pltpu.VMEM((m, s), BF)], name="weight_back")[0]


def _tall_back_body(a_ref, b_ref, out_ref, *, cut, n):
    res = _low(_nn(a_ref[...].T, b_ref[...]))
    for j in range(res.shape[0] // cut):
        out_ref[:, j * n : (j + 1) * n] = res[j * cut : (j + 1) * cut, :]


def tall_back(a, b, cut, tall):
    (s, m), n = a.shape, b.shape[1]
    rows, columns = m * cut // tall, n * tall // cut
    return _call(functools.partial(_tall_back_body, cut=cut, n=n), (m // tall,),
                 [(a, pl.BlockSpec((s, tall), lambda j: (0, j))), (b, pl.BlockSpec((s, n), lambda j: (0, 0), pipeline_mode=pl.Buffered(1)))],
                 [((rows, columns), BF, pl.BlockSpec((cut, columns), lambda j: (j, 0)))], 2 * s * m * n, name="tall_back")[0]


def _pack_body(*refs, plan):
    count = sum(len(p) for p in plan)
    ins, outs = refs[:count], refs[count:]
    at = 0
    for out, parts in zip(outs, plan):
        column = 0
        for _ in parts:
            ref = ins[at]
            at += 1
            rows, n = out.shape[0], ref.shape[2]
            for j in range(ref.shape[1] // rows):
                out[:, column : column + n] = ref[0, j * rows : (j + 1) * rows, :]
                column += n


def packed(plan, cut):
    flat = [p for parts in plan for p in parts]
    ins = [(w, pl.BlockSpec((1, *w.shape[1:]), lambda i, at=layer: (at, 0, 0))) for w, layer in flat]
    wide = [sum(w.shape[1] * w.shape[2] // cut for w, _ in parts) for parts in plan]
    return _call(functools.partial(_pack_body, plan=plan), (1,), ins,
                 [((cut, n), BF, pl.BlockSpec((cut, n), lambda i: (0, 0))) for n in wide], 0, name="pack")


def squares(g, so_far):
    tile = pl.BlockSpec((8, 128), lambda i: (0, 0))
    wide = min(g.shape[1], 2048)
    return _call(_squares_grid_body, (g.shape[1] // wide,), [(g, pl.BlockSpec((g.shape[0], wide), lambda i: (0, i))), (so_far, tile)],
                 [((8, 128), F32, tile)], 2 * g.size, name="squares")[0]


def _squares_grid_body(g_ref, so_far_ref, out_ref):
    @pl.when(pl.program_id(0) == 0)
    def _():
        out_ref[...] = so_far_ref[...]

    total = out_ref[...]
    for r in range(0, g_ref.shape[0], 16):
        g = g_ref[r : r + 16, :].astype(F32)
        g = g * g
        row = g[:8] + g[8:]
        parts = [row[:, c : c + 128] for c in range(0, row.shape[1], 128)]
        while len(parts) > 1:
            parts = [x + y for x, y in zip(parts[::2], parts[1::2])]
        total = total + parts[0]
    out_ref[...] = total


def _factor_body(own_ref, out_ref, held, send_sem, recv_sem, *, n, count):
    rep, me = lax.axis_index("rep"), lax.axis_index("dp")
    others = [(rep, lax.rem(me + k, n)) for k in range(1, n)]
    barrier = pltpu.get_barrier_semaphore()
    for other in others:
        pl.semaphore_signal(barrier, inc=1, device_id=other, device_id_type=pl.DeviceIdType.MESH)
    pl.semaphore_wait(barrier, n - 1)
    copies = [pltpu.make_async_remote_copy(src_ref=own_ref, dst_ref=held.at[k], send_sem=send_sem.at[k], recv_sem=recv_sem.at[k],
                                           device_id=other, device_id_type=pl.DeviceIdType.MESH) for k, other in enumerate(others)]
    for copy in copies:
        copy.start()
    for copy in copies:
        copy.wait()
    total = own_ref[...]
    for k in range(n - 1):
        total = total + held[k]
    total = jnp.sum(jnp.sum(total, axis=0, keepdims=True), axis=1, keepdims=True)
    out_ref[...] = jnp.broadcast_to(jnp.minimum(1.0, 0.5 * lax.rsqrt(total / count + 1e-30)), out_ref.shape)


def clip_factor(own, n, count):
    return pl.pallas_call(
        functools.partial(_factor_body, n=n, count=count),
        out_shape=jax.ShapeDtypeStruct((8, 128), F32),
        in_specs=[pl.BlockSpec(memory_space=pltpu.VMEM)],
        out_specs=pl.BlockSpec(memory_space=pltpu.VMEM),
        scratch_shapes=[pltpu.VMEM((n - 1, 8, 128), F32), pltpu.SemaphoreType.DMA((n - 1,)), pltpu.SemaphoreType.DMA((n - 1,))],
        compiler_params=pltpu.CompilerParams(collective_id=0, has_side_effects=True),
        cost_estimate=pl.CostEstimate(flops=10**6, transcendentals=0, bytes_accessed=65536),
        name="clip_factor",
    )(own)


def _adamw_body(*refs, n, f, tall):
    factor_ref, sums, rest = refs[0], refs[1:7], refs[7:]
    ins, outs = rest[:21], rest[21:]
    first = pl.program_id(0) == 0
    factor = factor_ref[0:1, 0:1]
    g_of = lambda i, columns: jnp.where(first, sums[i][:, columns], sums[3 + i][:, columns]).astype(F32)
    pieces = lambda k: [slice(at + k * tall, at + (k + 1) * tall) for at in range(0, 2 * f, 2 * tall)]
    where = [(0, [slice(i * n, (i + 1) * n)]) for i in range(4)] + [(1, pieces(0)), (1, pieces(1)), (2, [slice(None)])]
    for i, (which, columns) in enumerate(where):
        w, m, v = (ins[i + 7 * k][0].astype(F32) for k in range(3))
        g = jnp.concatenate([g_of(which, piece) for piece in columns], axis=1) * factor
        m = 0.9 * m + 0.1 * g
        v = 0.95 * v + 0.05 * g * g
        outs[i][0] = _low(w - 0.02 * (m * lax.rsqrt(v + 1e-8) + 0.1 * w))
        outs[7 + i][0] = m
        outs[14 + i][0] = v


def adamw(factor, sums, weights, m, v):
    n, f = weights[0].shape[2], weights[4].shape[2]
    cut, tall = weights[0].shape[1], weights[6].shape[1]
    steps = 4
    per, half = tall // steps, cut * steps // tall

    def block(a):
        return pl.BlockSpec((1, a.shape[1] // steps, a.shape[2]), lambda l, t: (l, t, 0))

    def held(layer, i, a):
        at = lambda l, t: jnp.where(l == layer, t, (1 - layer) * (steps - 1))
        if i == 2:
            return pl.BlockSpec((per, n), lambda l, t: (lax.rem(at(l, t), half), lax.div(at(l, t), half)))
        return pl.BlockSpec((a.shape[0] // steps, a.shape[1]), lambda l, t: (at(l, t), 0))

    arrays = (*weights, *m, *v)
    ins = [(factor, pl.BlockSpec((8, 128), lambda l, t: (0, 0)))]
    ins += [(a, held(layer, i, a)) for layer in range(2) for i, a in enumerate(sums[layer])]
    ins += [(a, block(a)) for a in arrays]
    return _call(functools.partial(_adamw_body, n=n, f=f, tall=tall), (2, steps), ins, [(a.shape, a.dtype, block(a)) for a in arrays], 10**8, name="adamw")


def solution(mesh):
    def gathered(w):
        return lax.all_gather(w, "dp", axis=0, tiled=True)

    def scattered(g):
        return lax.psum_scatter(g, "dp", scatter_dimension=0, tiled=True)

    def step(x, dy, *arrays):
        weights, m, v = (arrays[i : i + 7] for i in (0, 7, 14))
        s, d = x.shape[1:]
        n, f = weights[0].shape[2], weights[4].shape[2]
        cut, tall = weights[0].shape[1], weights[6].shape[1]
        tie = lambda *xs: lax.optimization_barrier(xs)

        (p0,) = packed([[(weights[i], 0) for i in range(4)]], cut)
        rest = packed([[(weights[4], 0), (weights[5], 0)], [(weights[6], 0)] + [(weights[i], 1) for i in range(4)],
                       [(weights[4], 1), (weights[5], 1)], [(weights[6], 1)]], cut)
        w0, w1, w2, w3, w4 = (gathered(p) for p in (p0, *rest))
        full = [dict(w_gate=(gu, d, f, 0), w_up=(gu, d, f, 1), w_down=(down, d, f, 0),
                     **{name: (qkvo, d, n, first + i) for i, name in enumerate(NAMES[:4])})
                for gu, down, qkvo, first in ((w1, w2, w0, 0), (w3, w4, w2, 4))]

        angle = jnp.arange(s, dtype=F32)[:, None] * THETA ** (-jnp.arange(HALF, dtype=F32) / HALF)
        cos, sin = jnp.cos(angle), jnp.sin(angle)

        h, kept = x[0], []
        for w in full:
            a, q, k, vv = fwd_qkv(h, cos, sin, w["wq"], w["wk"], w["wv"])
            o, lse = attend(q, k, vv)
            h2, b = fwd_out(o, h, w["wo"])
            act, by_up, by_gate = fwd_gate_up(b, w["w_gate"], w["w_up"])
            kept.append((h, a, q, k, vv, o, lse, h2, b, act, by_up, by_gate))
            if w is not full[-1]:
                h = fwd_down(act, h2, w["w_down"], cut)

        by_h = dy[0]
        for number in (1, 0):
            w = full[number]
            h, a, q, k, vv, o, lse, h2, b, act, by_up, by_gate = kept[number]
            g_down = tall_back(act, by_h, cut, tall)
            g_down, by_h = tie(g_down, by_h)
            s_down = scattered(g_down)
            if number == 0:
                s_gu1, by_up = tie(s_gu, by_up)
            dg, du, g_gu = units_back(by_h, b, by_up, by_gate, w["w_down"], cut, tall)
            if number == 0:
                s_qkvo1, g_gu, dg = tie(s_qkvo, g_gu, dg)
            else:
                g_gu, dg = tie(g_gu, dg)
            s_gu = scattered(g_gu)
            dh, do, delta = mlp_back(dg, du, by_h, h2, o, w["w_gate"], w["w_up"], w["wo"])
            dq, dk, dv = attend_back(q, k, vv, do, lse, delta, cos, sin)
            s_down, dq = tie(s_down, dq)
            g_qkvo = weight_back([(a, dq), (a, dk), (a, dv), (o, dh)])
            if number:
                g_qkvo, dq = tie(g_qkvo, dq)
                s_down1 = s_down
                by_h = qkv_back(dq, dk, dv, h, dh, w["wq"], w["wk"], w["wv"])
            else:
                s_gu, g_qkvo = tie(s_gu, g_qkvo)
            s_qkvo = scattered(g_qkvo)
        sums = ((s_qkvo, s_gu, s_down), (s_qkvo1, s_gu1, s_down1))
        total = jnp.zeros((8, 128), F32)
        for g in (s_down1, s_gu1, s_qkvo1, s_down, s_gu, s_qkvo):
            total = squares(g, total)
        size = mesh.shape["dp"]
        factor = clip_factor(total, size, float(size * sum(g.size for layer in sums for g in layer)))
        return tuple(adamw(factor, sums, weights, m, v))

    states, rows = P(("rep", "dp"), None, None), P(None, "dp", None)
    return jax.shard_map(
        step,
        mesh=mesh,
        in_specs=(states, states) + (rows,) * 21,
        out_specs=(P("rep", "dp", None),) * 21,
        check_vma=False,
    )
```
